512 devices in a mesh: dp: 128 (over y, z, core), mp: 4 (over x).
Axes of the slice: x: 4, y: 8, z: 8, core: 2. Of those that a mesh axis runs over, the one named last changes fastest.
Arguments:
- gradient: bfloat16 [128, 64, 14336], P('dp', None, 'mp'), may hold values from -6 to 6
- momentum: float32 [128, 64, 14336], P('dp', None, 'mp'), may hold values from -6 to 6
- weights: float32 [64, 14336], P(None, 'mp'), may hold values from -6 to 6
- positions: int32 [128, 1, 224, 32], P('dp', None, 'mp'), may hold values from 0 to 4095, as said below
Outputs:
- new_momentum: float32 [128, 64, 14336], P('dp', None, 'mp')
- new_weights: float32 [64, 14336], P(None, 'mp')
The draws below stay inside these ranges and needn't reach their ends.
Inputs may be any that keep to these rules, and one draw needn't show every extreme that they name: Within one span of one replica the 32 positions are all different.
All inputs are finite; a program needn't handle non-finite values.
Results may differ from the reference program's by a relative error of at most 0.0003.
Values sent between devices are 32-bit elements; how exact they have to be, the bound alone decides.
A program may use at most 64 MiB of HBM per device.

```python
import jax
import jax.numpy as jnp
from jax import lax

FF = 14336
BANDS = 1
K = 32
REPLICAS = 128
COLCH = 224


def draw_positions(key, part):
    scores = jax.random.randint(key, (REPLICAS, BANDS, FF // 64, 4096), 0, 262144, dtype=jnp.int32)
    scores = scores * 4096 + jnp.arange(4096, dtype=jnp.int32)
    chosen = jax.lax.top_k(scores, K)[1]
    return chosen.astype(jnp.int32)


def levels(own_key, dims, split, least, top_value):
    level, own = 1.0, jax.random.fold_in(own_key, 6)
    for dim, blocks in split:
        heights = jnp.exp(jax.random.uniform(jax.random.fold_in(own, dim), (blocks,), jnp.float32, least / len(split), top_value / len(split)))
        level = level * jnp.repeat(heights, dims[dim] // blocks).reshape([-1 if axis == dim else 1 for axis in range(len(dims))])
    return level


def normal_values(rng, extent, scale, most, shards=(), held_as=jnp.bfloat16):
    result = scale * jax.random.normal(rng, extent, jnp.float32)
    if shards:
        result = result * levels(rng, extent, shards, -0.22, 0.18)
    return jnp.clip(result, -most, most).astype(held_as)


def setup_inputs(seed: int = 0) -> dict:
    splits = jax.random.split(jax.random.key(seed), 5)
    gradient = normal_values(splits[0], (REPLICAS, 64 * BANDS, FF), 1.0, 6.0, ((0, 128), (2, 4)))
    momentum = normal_values(splits[1], (REPLICAS, 64 * BANDS, FF), 1.0, 6.0, ((0, 128), (2, 4)), jnp.float32)
    weights = normal_values(splits[2], (64 * BANDS, FF), 1.0, 6.0, ((1, 4),), jnp.float32)
    positions = draw_positions(jax.random.fold_in(splits[4], 71), 0)
    return {"gradient": gradient, "momentum": momentum, "weights": weights, "positions": positions}


def dct_table():
    column = jnp.arange(64, dtype=jnp.float32)
    freq = column[:, None]
    factor = jnp.where(freq == 0, jnp.sqrt(jnp.float32(1.0 / 64)), jnp.sqrt(jnp.float32(2.0 / 64)))
    return factor * jnp.cos(jnp.pi * (2.0 * column[None, :] + 1.0) * freq / 128.0)

def reference(gradient, momentum, weights, positions):
    table = dct_table()
    rows_all = 64 * BANDS
    band_index = jnp.arange(BANDS, dtype=jnp.int32)[:, None, None]
    span_index = jnp.arange(COLCH, dtype=jnp.int32)[None, :, None]

    def one_replica(carry, inputs):
        grad_one, mom_one, pos_one = inputs
        summed = 0.9 * mom_one + grad_one.astype(jnp.float32)
        blocks = summed.reshape(BANDS, 64, COLCH, 64)
        coefs = jnp.einsum('kr,brcs,ls->bckl', table, blocks, table, precision=lax.Precision.HIGHEST)
        flatten = coefs.reshape(BANDS, COLCH, 4096)
        picked = jnp.take_along_axis(flatten, pos_one, axis=2)
        own = jnp.zeros((BANDS, COLCH, 4096), jnp.float32).at[band_index, span_index, pos_one].add(picked)
        back = jnp.einsum('kr,bckl,ls->brcs', table, own.reshape(BANDS, COLCH, 64, 64), table, precision=lax.Precision.HIGHEST)
        return (carry + own, summed - back.reshape(rows_all, FF))
    start = jnp.zeros((BANDS, COLCH, 4096), jnp.float32)
    aggregate, new_momentum = lax.scan(one_replica, start, (gradient, momentum, positions))
    update = jnp.einsum('kr,bckl,ls->brcs', table, aggregate.reshape(BANDS, COLCH, 64, 64), table, precision=lax.Precision.HIGHEST)
    update = update.reshape(rows_all, FF)
    meansq = jnp.mean(update * update)
    new_weights = weights - update / jnp.sqrt(meansq + 1.0)
    return (new_momentum, new_weights)
```

```python
import functools

import jax
import jax.numpy as jnp
import numpy as np
from jax import lax
from jax.experimental import pallas as pl
from jax.experimental.pallas import tpu as pltpu
from jax.sharding import Mesh
from jax.sharding import PartitionSpec as P

MESH = pl.DeviceIdType.MESH
FF = 14336
DP = ("y", "z", "c")
F32 = jnp.float32
BF16 = jnp.bfloat16
NT = (((1,), (1,)), ((), ()))
NN = (((1,), (0,)), ((), ()))
BLOCK = 512
SPANS = 56
GROUPS = SPANS // 4


def dct_parts():
    n = np.arange(64, dtype=np.float64)
    scale = np.where(n == 0, np.sqrt(1.0 / 64), np.sqrt(2.0 / 64))[:, None]
    table = scale * np.cos(np.pi * (2.0 * n[None, :] + 1.0) * n[:, None] / 128.0)
    high = table.astype(BF16)
    low = (table - high.astype(np.float64)).astype(BF16)
    return high, low


def split2(x):
    high = x.astype(BF16)
    return high, (x - high.astype(F32)).astype(BF16)


def dot(a, b, dims=NN):
    return lax.dot_general(a, b, dims, preferred_element_type=F32)


def local_kernel(g_ref, m_ref, pos_ref, lookup_ref, new_ref, msg_ref, places, picks):
    step = pl.program_id(0)

    @pl.when(step == 0)
    def _():
        places[...] = jnp.concatenate(
            [pos_ref[pl.ds(c, GROUPS, stride=4), :] for c in range(4)], axis=1
        )

    summed = 0.9 * m_ref[0] + g_ref[0].astype(F32)
    freqs = lax.broadcasted_iota(jnp.int32, (64, 128), 0)
    span_of_lane = lax.broadcasted_iota(jnp.int32, (64, 128), 1) // 32
    for q in range(BLOCK // 256):
        group = step * (BLOCK // 256) + q
        place = places[pl.ds(group, 1), :]
        hot = jnp.concatenate([freqs == place // 64, freqs == place % 64], axis=1)
        looked = dot(lookup_ref[...], hot.astype(F32).astype(BF16))
        rows = looked[:64, :128] + looked[64:, :128]
        col_high = jnp.concatenate(
            [jnp.where(span_of_lane == c, looked[:64, 128:], 0.0) for c in range(4)], axis=0
        ).astype(BF16)
        col_low = jnp.concatenate(
            [jnp.where(span_of_lane == c, looked[64:, 128:], 0.0) for c in range(4)], axis=0
        ).astype(BF16)
        field = summed[:, q * 256 : (q + 1) * 256]
        high, low = split2(field)
        mixed = dot(high, col_high) + dot(low, col_high) + dot(high, col_low)
        picked = jnp.sum(rows * mixed, axis=0, keepdims=True)
        picks[pl.ds(group, 1), :] = picked
        high, low = split2(rows * picked)
        back = dot(high, col_high, NT) + dot(low, col_high, NT) + dot(high, col_low, NT)
        new_ref[0, :, q * 256 : (q + 1) * 256] = field - back

    @pl.when(step == pl.num_programs(0) - 1)
    def _():
        lane = lax.broadcasted_iota(jnp.int32, (GROUPS, 128), 1)
        values, where = picks[...], places[...].astype(F32)
        for c in range(4):
            left = values if c == 0 else pltpu.roll(values, 128 - 32 * c, 1)
            right = where if c == 1 else pltpu.roll(where, (32 - 32 * c) % 128, 1)
            row = jnp.where(lane < 32, left, jnp.where(lane < 64, right, 0.0))
            for g in range(GROUPS):
                span = 4 * g + c
                msg_ref[span // 7, span % 7] = row[g : g + 1, :]
        for y in range(8):
            msg_ref[y, 7] = jnp.zeros((1, 128), F32)


def local_step(gradient, momentum, positions, lookup):
    width = momentum.shape[2]
    return pl.pallas_call(
        local_kernel,
        grid=(width // BLOCK,),
        in_specs=[
            pl.BlockSpec((1, 64, BLOCK), lambda i: (0, 0, i)),
            pl.BlockSpec((1, 64, BLOCK), lambda i: (0, 0, i)),
            pl.BlockSpec((SPANS, 32), lambda i: (0, 0)),
            pl.BlockSpec((128, 64), lambda i: (0, 0)),
        ],
        out_specs=[
            pl.BlockSpec((1, 64, BLOCK), lambda i: (0, 0, i)),
            pl.BlockSpec((8, 8, 1, 128), lambda i: (0, 0, 0, 0)),
        ],
        out_shape=[
            jax.ShapeDtypeStruct((1, 64, width), F32),
            jax.ShapeDtypeStruct((8, 8, 1, 128), F32),
        ],
        scratch_shapes=[pltpu.VMEM((GROUPS, 128), jnp.int32), pltpu.VMEM((GROUPS, 128), F32)],
    )(gradient, momentum, positions, lookup)


def aggregate_span(rows):
    flat = rows.T
    values, where = flat[:32], flat[32:64]
    row_freq = jnp.floor(where * (1.0 / 64.0))
    col_freq = where - 64.0 * row_freq
    freqs = lax.broadcasted_iota(jnp.int32, (64, 128), 0).astype(F32)
    lefts, rights = [], []
    for j in range(32):
        put = jnp.where(freqs == row_freq[j : j + 1], values[j : j + 1], 0.0)
        high, low = split2(put)
        lefts.append(jnp.concatenate([high, low], axis=0))
        rights.append(jnp.where(freqs == col_freq[j : j + 1], 1.0, 0.0).astype(BF16))
    both = dot(jnp.concatenate(lefts, axis=1), jnp.concatenate(rights, axis=1), NT)
    return both[:64] + both[64:]


def exchange_kernel(
    msg_ref, q_ref, qt_ref, upd_ref, den_ref,
    r1, r2, ag, xs,
    s1, t1, s2, t2, s3, t3, s4, t4, s5, t5, s6, t6,
):
    y, z, c, mp = (lax.axis_index(n) for n in ("y", "z", "c", "mp"))

    def device(ty, tz, tc, tmp):
        return {"y": ty, "z": tz, "c": tc, "mp": tmp}

    def send(src, dst, ssem, rsem, to):
        return pltpu.make_async_remote_copy(
            src_ref=src, dst_ref=dst, send_sem=ssem, recv_sem=rsem,
            device_id=to, device_id_type=MESH,
        )

    barrier = pltpu.get_barrier_semaphore()
    peers = [device(lax.rem(y + d, 8), z, c, mp) for d in range(1, 8)]
    peers += [device(y, lax.rem(z + d, 8), lax.rem(c + e, 2), mp) for d in range(8) for e in range(2) if d or e]
    peers += [device(y, z, c, lax.rem(mp + d, 4)) for d in range(1, 4)]
    for peer in peers:
        pl.semaphore_signal(barrier, inc=1, device_id=peer, device_id_type=MESH)
    pl.semaphore_wait(barrier, len(peers))

    far = (4, 3, 5, 2, 6, 1, 7)
    near = (1, 7, 2, 6, 3, 5, 4)

    first = {}
    for d in far:
        ty = lax.rem(y + d, 8)
        first[d] = send(msg_ref.at[ty], r1.at[y], s1.at[d], t1.at[d], device(ty, z, c, mp))
        first[d].start()
    r1[y] = msg_ref[y]
    for d in near:
        first[d].wait_recv()

    second = {}
    for d in far + (0,):
        for e in range(2):
            if d or e:
                tz, tc = lax.rem(z + d, 8), lax.rem(c + e, 2)
                second[d, e] = send(
                    r1.at[:, tz], r2.at[z * 2 + c], s2.at[d, e], t2.at[d, e], device(y, tz, tc, mp)
                )
                second[d, e].start()
    r2[z * 2 + c] = r1[:, z]
    for d in (0,) + near:
        for e in range(2):
            if d or e:
                second[d, e].wait_recv()

    rows = jnp.concatenate([r2[i, :, 0, :] for i in range(16)], axis=0)
    total = aggregate_span(rows)
    high, low = split2(total)
    wide = dot(high, q_ref[0]) + dot(low, q_ref[0]) + dot(high, q_ref[1])
    high, low = split2(wide)
    qt = qt_ref[c]
    part = dot(qt[0], high) + dot(qt[0], low) + dot(qt[1], high)
    a = y + c * (z - y)
    b = z + c * (y - z)
    ag[c, a, b] = jnp.concatenate([part[:16], part[16:]], axis=1)

    def along_b(to):
        return device(y + c * (to - y), z + (1 - c) * (to - z), c, mp)

    def along_a(to):
        return device(y + (1 - c) * (to - y), z + c * (to - z), c, mp)

    third = {}
    for d in far:
        to = lax.rem(b + d, 8)
        third[d] = send(ag.at[c, a, b], ag.at[c, a, b], s3.at[d], t3.at[d], along_b(to))
        third[d].start()

    def fan_out(slot):
        for d in far:
            to = lax.rem(a + d, 8)
            send(ag.at[c, a, slot], ag.at[c, a, slot], s4.at[d], t4.at[d], along_a(to)).start()

    fan_out(b)
    for d in near:
        third[d].wait_recv()
        fan_out(lax.rem(b + 8 - d, 8))

    def whole(ref, sem):
        return pltpu.make_async_copy(ref, ref, sem)

    fifth = {}
    for d in (0,) + near:
        frm = lax.rem(a + 8 - d, 8)
        if d:
            whole(ag.at[c, frm], t4.at[d]).wait()
        fifth[d] = send(ag.at[c, frm], ag.at[c, frm], s5.at[d], t5.at[d], device(y, z, 1 - c, mp))
        fifth[d].start()
    for d in (0,) + near:
        fifth[d].wait_recv()

    lane = lax.broadcasted_iota(jnp.int32, (16, 128), 1)
    square = jnp.zeros((16, 128), F32)
    for q in range(SPANS // 2):
        for h in range(2):
            pair = []
            for span in (2 * q, 2 * q + 1):
                k, i = span // 7, span % 7
                pair.append(ag[0, k, i] if h == 0 else ag[1, i, k])
            even, odd = pair
            top = jnp.where(lane < 64, even, pltpu.roll(odd, 64, 1))
            low = jnp.where(lane < 64, pltpu.roll(even, 64, 1), odd)
            upd_ref[h * 32 : h * 32 + 16, q * 128 : (q + 1) * 128] = top
            upd_ref[h * 32 + 16 : h * 32 + 32, q * 128 : (q + 1) * 128] = low
            square += top * top + low * low

    xs[mp] = square
    sixth = {}
    for d in range(1, 4):
        to = lax.rem(mp + d, 4)
        sixth[d] = send(xs.at[mp], xs.at[mp], s6.at[d], t6.at[d], device(y, z, c, to))
        sixth[d].start()
    for d in range(1, 4):
        sixth[d].wait_recv()
    meansq = jnp.sum(xs[...]) / (64.0 * FF)
    den_ref[...] = jnp.sqrt(jnp.full((8, 128), meansq + 1.0, F32))

    for d in near:
        first[d].wait_send()
        third[d].wait_send()
        whole(ag.at[c, a], s4.at[d]).wait()
    for key in second:
        second[key].wait_send()
    for key in fifth:
        fifth[key].wait_send()
    for key in sixth:
        sixth[key].wait_send()


def exchange(msg, q, qt, width):
    dma = pltpu.SemaphoreType.DMA
    vmem = pl.BlockSpec(memory_space=pltpu.VMEM)
    return pl.pallas_call(
        exchange_kernel,
        in_specs=[vmem] * 3,
        out_specs=[vmem] * 2,
        out_shape=[jax.ShapeDtypeStruct((64, width), F32), jax.ShapeDtypeStruct((8, 128), F32)],
        scratch_shapes=[
            pltpu.VMEM((8, 8, 1, 128), F32),
            pltpu.VMEM((16, 8, 1, 128), F32),
            pltpu.VMEM((2, 8, 8, 16, 128), F32),
            pltpu.VMEM((4, 16, 128), F32),
            dma((8,)), dma((8,)), dma((8, 2)), dma((8, 2)), dma((8,)), dma((8,)),
            dma((8,)), dma((8,)), dma((8,)), dma((8,)), dma((4,)), dma((4,)),
        ],
        compiler_params=pltpu.CompilerParams(collective_id=0, has_side_effects=True),
    )(msg, q, qt)


def local(gradient, momentum, weights, positions):
    high, low = dct_parts()
    lookup = jnp.asarray(np.concatenate([high.T, low.T], axis=0))
    q = jnp.asarray(np.stack([high, low]))
    qt = jnp.asarray(np.stack([np.stack([high.T[32 * p : 32 * p + 32], low.T[32 * p : 32 * p + 32]]) for p in range(2)]))
    new_momentum, msg = local_step(gradient, momentum, positions.reshape(SPANS, 32), lookup)
    update, den = exchange(msg, q, qt, weights.shape[1])
    new_weights = weights - update / den[0, 0]
    return (new_momentum, new_weights)


def solution(mesh):
    torus = Mesh(mesh.devices.reshape(8, 8, 2, mesh.shape["mp"]), ("y", "z", "c", "mp"))
    in_specs = (P(DP, None, "mp"), P(DP, None, "mp"), P(None, "mp"), P(DP, None, "mp", None))
    out_specs = (P(DP, None, "mp"), P(None, "mp"))
    return jax.shard_map(local, mesh=torus, in_specs=in_specs, out_specs=out_specs, check_vma=False)
```
